32 devices in a mesh: seq: 8 (over y, x, core), vocab: 4 (over z).
Axes of the slice: x: 2, y: 2, z: 4, core: 2. Of those that a mesh axis runs over, the one named last changes fastest.
Arguments:
- hidden: bfloat16 [960, 4096], P('seq'), may hold values from -32 to 32
- head_weight: bfloat16 [4096, 98304], P(None, ('seq', 'vocab')), may hold values from -0.84375 to 0.84375
- labels: int32 [960], P('seq'), may hold values from 0 to 98303
- lengths: int32 [8], replicated, may hold values from 1 to 120, 480 in all
- pair_map: int32 [8], replicated, may hold values from 0 to 7, each once
- ref_margin: float32 [4], replicated, may hold values from -240 to 240
Outputs:
- seq_logps: float32 [8], replicated
- pair_loss: float32 [4], replicated
- z_loss: float32 [], replicated
The draws below stay inside these ranges and needn't reach their ends.
Inputs may be any that keep to these rules, and one draw needn't show every extreme that they name: The lengths sum to 480 and the longest is exactly 120. Each response appears once; pair p compares response pair_map[2p], chosen, with response pair_map[2p+1], rejected.
All inputs are finite; a program needn't handle non-finite values.
Results may differ from the reference program's by a relative error of at most 0.0003.
Values may be sent and summed in bfloat16 or wider, within the bound.
No kernel may reach another device: no remote copies, remote signals or barrier semaphores. Data moves between devices by JAX's collectives and lax.ppermute only.
A program may use at most 192 MiB of HBM per device.

```python
import math
import jax
import jax.numpy as jnp
import numpy as np
from jax import lax

D = 4096
VOCAB = 98304
TOK_DEV = 120
SEQS = 8
PAIRS = 4
TOKENS = 960


def draw_hidden(key, part):
    values_out = jnp.clip(jax.random.normal(jax.random.fold_in(key, 1), (TOKENS, D), jnp.float32), -6.0, 6.0)
    return jnp.clip(values_out, -32.0, 32.0).astype(jnp.bfloat16)


def draw_head_weight(key, part):
    weight_scale = 3.0 / math.sqrt(D)
    values_out = jnp.clip(jax.random.normal(jax.random.fold_in(key, 3), (D, VOCAB), jnp.float32), -6.0, 6.0) * weight_scale
    return values_out.astype(jnp.bfloat16)


def with_ends(values, key, smallest, top_value):
    place = [jax.random.randint(jax.random.fold_in(key, axis), (), 0, length) for axis, length in enumerate(values.shape)]
    main_axis = values.shape.index(max(values.shape))
    next_to = place[:main_axis] + [(place[main_axis] + 1) % values.shape[main_axis]] + place[main_axis + 1:]
    return values.at[tuple(place)].set(smallest).at[tuple(next_to)].set(top_value)


def profile(amount, total, reach, skew):
    weights = [(1 << 20) // math.isqrt(grade ** skew) + 1 for grade in range(2, amount + 1)]
    rest, holding = total - reach - (amount - 1), [1] * (amount - 1)
    while rest > 0:
        candidates = [i for i in range(amount - 1) if holding[i] < reach]
        pool, left = sum([weights[i] for i in candidates]), rest
        for i in candidates:
            addition = min(reach - holding[i], max(1, left * weights[i] // pool), rest)
            holding[i] = holding[i] + addition
            rest = rest - addition
    return np.array([reach] + holding)


def ragged_sizes(stream_key, number_of, total, bound, lean):
    if number_of == 2:
        one = jax.random.randint(stream_key, (), max(1, total - bound), min(bound, total - 1) + 1)
        return jnp.stack([one, total - one])
    sizes = jnp.asarray(profile(number_of, total, bound, lean), jnp.int32)
    pairs = (number_of - 1) // 2
    source_of, sink = sizes[1:1 + 2 * pairs:2], sizes[2:2 + 2 * pairs:2]
    room = jnp.minimum(source_of - 1, bound - sink)
    shifted = jax.random.randint(jax.random.fold_in(stream_key, 1), (pairs,), 0, 1 << 20) % (room + 1)
    sizes = sizes.at[1:1 + 2 * pairs:2].set(source_of - shifted).at[2:2 + 2 * pairs:2].set(sink + shifted)
    return sizes[jax.random.permutation(jax.random.fold_in(stream_key, 2), number_of)]


def centred(rng, extent, deviation, most, held_as=jnp.bfloat16):
    return jnp.clip(deviation * jax.random.normal(rng, extent, jnp.float32), -most, most).astype(held_as)


def setup_inputs(seed: int = 0) -> dict:
    key_list = jax.random.split(jax.random.key(seed), 7)
    hidden = draw_hidden(jax.random.fold_in(key_list[6], 71), 0)
    head_weight = draw_head_weight(jax.random.fold_in(key_list[6], 71), 0)
    labels = with_ends(jax.random.randint(key_list[2], (TOKENS,), 0, VOCAB), jax.random.fold_in(key_list[2], 1), 0, VOCAB - 1).astype(jnp.int32)
    lengths = ragged_sizes(key_list[3], SEQS, TOKENS // 2, TOK_DEV, 2).astype(jnp.int32)
    pair_map = jax.random.permutation(key_list[4], SEQS).astype(jnp.int32)
    ref_margin = centred(key_list[5], (PAIRS,), 40.0, 240.0, jnp.float32)
    return dict(hidden=hidden, head_weight=head_weight, labels=labels, lengths=lengths, pair_map=pair_map, ref_margin=ref_margin)


pref_beta = 0.05
zloss_weight = 0.0001


def reference(hidden, head_weight, labels, lengths, pair_map, ref_margin):
    def per_sequence(seq_items):
        row_block, label_ids = seq_items
        logits = jnp.dot(row_block, head_weight, preferred_element_type=jnp.float32)
        log_norm = jax.nn.logsumexp(logits, axis=1)
        picked = jnp.take_along_axis(logits, label_ids[:, None], axis=1)[:, 0]
        return log_norm, picked

    log_norm, picked = lax.map(per_sequence, (hidden.reshape(SEQS, TOK_DEV, D), labels.reshape(SEQS, TOK_DEV)))
    live_mask = jnp.arange(TOK_DEV, dtype=jnp.int32)[None, :] < lengths[:, None]
    seq_logps = jnp.sum(jnp.where(live_mask, picked - log_norm, 0.0), axis=1)
    chosen = seq_logps[pair_map[0::2]]
    rejected = seq_logps[pair_map[1::2]]
    pair_loss = jax.nn.softplus(-pref_beta * (chosen - rejected - ref_margin))
    live_count = jnp.sum(live_mask.astype(jnp.float32))
    z_loss = zloss_weight * jnp.sum(jnp.where(live_mask, log_norm * log_norm, 0.0)) / live_count
    return seq_logps, pair_loss, z_loss
```

```python
import functools

import jax
import jax.numpy as jnp
from jax import lax
from jax.experimental import pallas as pl
from jax.experimental.pallas import tpu as pltpu
from jax.sharding import PartitionSpec as P

pref_beta = 0.05
zloss_weight = 0.0001
LANES = 128
STRIPE = 8
NEG = -1e30


def softplus(x):
    return jnp.maximum(x, 0.0) + jnp.log1p(jnp.exp(-jnp.abs(x)))


def head_kernel(metas, depth, block, first, lens_ref, w_in, prev_ref, *rest):
    pieces = rest[: len(metas)]
    if first:
        slab_ref, w_ref = rest[len(metas) : len(metas) + 2]
        scratch = rest[len(metas) + 2 :]
    else:
        slab_ref, w_ref = rest[len(metas)], w_in
        scratch = rest[len(metas) + 1 :]
    x_buf, logit_buf, m_buf, s_buf, p_buf, lab_buf, lse_col, pick_col, x_sem, w_sem = scratch
    responses = lens_ref.shape[0]
    rows_max = x_buf.shape[0]
    columns = w_ref.shape[1]
    steps = columns // block
    me = lax.axis_index("seq")
    col_first = (me * lax.axis_size("vocab") + lax.axis_index("vocab")) * columns

    def w_copy(n):
        cols = pl.ds(pl.multiple_of(n * block, block), block)
        return pltpu.make_async_copy(w_in.at[:, cols], w_ref.at[:, cols], w_sem.at[n])

    offs, counts, total = [], [], jnp.int32(0)
    for rel, pos, rows in metas:
        live = jnp.clip(lens_ref[me ^ rel] - pos, 0, rows)
        offs.append(total)
        counts.append(live)
        total = total + (live + STRIPE - 1) // STRIPE

    def x_copy(j, b):
        src = pieces[j].at[pl.ds(pl.multiple_of(b * STRIPE, STRIPE), STRIPE), :]
        dst = x_buf.at[pl.ds(pl.multiple_of((offs[j] + b) * STRIPE, STRIPE), STRIPE), :]
        return pltpu.make_async_copy(src, dst, x_sem)

    for j in range(len(metas)):
        @pl.loop(0, (counts[j] + STRIPE - 1) // STRIPE)
        def _(b):
            x_copy(j, b).start()

    if first:
        for n in range(steps):
            w_copy(n).start()
        slab_ref[...] = jnp.zeros_like(slab_ref)
    else:
        slab_ref[...] = prev_ref[...]

    @pl.loop(0, total)
    def _(b):
        x_copy(0, 0).wait()

    def compute(rows):
        dig = x_buf[0:rows, depth : depth + LANES].astype(jnp.float32)
        lab = dig[:, 0:1] + 256.0 * dig[:, 1:2] + 65536.0 * dig[:, 2:3]
        lane = lax.broadcasted_iota(jnp.int32, (rows, LANES), 1)
        lab_buf[0:rows, :] = lab.astype(jnp.int32) - col_first - lane
        m_buf[0:rows, :] = jnp.full((rows, LANES), NEG, jnp.float32)
        s_buf[0:rows, :] = jnp.zeros((rows, LANES), jnp.float32)
        p_buf[0:rows, :] = jnp.zeros((rows, LANES), jnp.float32)
        logit_buf[1, 0:rows, :] = jnp.full((rows, block), NEG, jnp.float32)

        def reduce(slot, base):
            for r0 in range(0, rows, 16):
                r = slice(r0, r0 + min(16, rows - r0))
                groups = [logit_buf[slot, r, g : g + LANES] for g in range(0, block, LANES)]
                m_old = m_buf[r, :]
                m_new = m_old
                for a in groups:
                    m_new = jnp.maximum(m_new, a)
                s = s_buf[r, :] * jnp.exp(m_old - m_new)
                p, lr = p_buf[r, :], lab_buf[r, :]
                for g, a in enumerate(groups):
                    s = s + jnp.exp(a - m_new)
                    p = p + jnp.where(lr == base + g * LANES, a, 0.0)
                m_buf[r, :], s_buf[r, :], p_buf[r, :] = m_new, s, p

        @pl.loop(0, steps)
        def _(n):
            if first:
                w_copy(n).wait()
            slot = n % 2
            cols = pl.ds(pl.multiple_of(n * block, block), block)
            logit_buf[slot, 0:rows, :] = jnp.dot(
                x_buf[0:rows, 0:depth], w_ref[:, cols], preferred_element_type=jnp.float32
            )
            reduce(1 - slot, jnp.where(n == 0, 1 << 30, (n - 1) * block))

        reduce((steps - 1) % 2, (steps - 1) * block)
        m = m_buf[0:rows, :]
        top = jnp.max(m, axis=1, keepdims=True)
        total_exp = jnp.sum(s_buf[0:rows, :] * jnp.exp(m - top), axis=1, keepdims=True)
        lse_col[0:rows, :] = jnp.broadcast_to(top + jnp.log(total_exp), (rows, LANES))
        pick = jnp.sum(p_buf[0:rows, :], axis=1, keepdims=True)
        pick_col[0:rows, :] = jnp.broadcast_to(pick, (rows, LANES))

    sizes = sorted({r for r in (128, 192) if r < rows_max} | {rows_max})
    below = 0
    for size in sizes:
        @pl.when((total * STRIPE > below) & (total * STRIPE <= size))
        def _():
            compute(size)

        below = size
    if first:
        @pl.when(total == 0)
        def _():
            for n in range(steps):
                w_copy(n).wait()

    lane = lax.broadcasted_iota(jnp.int32, (1, LANES), 1)
    for j, (rel, pos, rows) in enumerate(metas):
        @pl.when(counts[j] > 0)
        def _():
            at = pl.ds(pl.multiple_of(offs[j] * STRIPE, STRIPE), LANES)
            here = (lane >= pos) & (lane < pos + counts[j])
            for base, col in ((0, lse_col), (responses, pick_col)):
                line = col[at, :].T[0:1, :]
                if pos:
                    line = pltpu.roll(line, pos, 1)
                out = pl.ds(base + (me ^ rel), 1)
                slab_ref[out, :] = slab_ref[out, :] + jnp.where(here, line, 0.0)


def head_call(metas, depth, block, lengths, w, prev, pieces, first):
    responses = lengths.shape[0]
    rows = sum(m[2] for m in metas)
    columns = w.shape[1]
    vmem, smem, any_ = (
        pl.BlockSpec(memory_space=pltpu.VMEM),
        pl.BlockSpec(memory_space=pltpu.SMEM),
        pl.BlockSpec(memory_space=pl.ANY),
    )
    slab = jax.ShapeDtypeStruct((2 * responses, LANES), jnp.float32)
    out_shape, out_specs = slab, vmem
    if first:
        out_shape, out_specs = (slab, pltpu.VMEM(w.shape, w.dtype)), (vmem, vmem)
    row_buf = pltpu.VMEM((rows, LANES), jnp.float32)
    col_buf = pltpu.VMEM((rows + LANES, LANES), jnp.float32)
    return pl.pallas_call(
        functools.partial(head_kernel, metas, depth, block, first),
        out_shape=out_shape,
        in_specs=[smem, any_ if first else vmem, vmem] + [any_] * len(pieces),
        out_specs=out_specs,
        scratch_shapes=[
            pltpu.VMEM((rows, pieces[0].shape[1]), jnp.bfloat16),
            pltpu.VMEM((2, rows, block), jnp.float32),
            row_buf,
            row_buf,
            row_buf,
            pltpu.VMEM((rows, LANES), jnp.int32),
            col_buf,
            col_buf,
            pltpu.SemaphoreType.DMA,
            pltpu.SemaphoreType.DMA((columns // block,)),
        ],
        compiler_params=pltpu.CompilerParams(vmem_limit_bytes=(12 if not first else 12) << 20),
        cost_estimate=pl.CostEstimate(
            flops=rows * depth * columns, bytes_accessed=4 << 20, transcendentals=0
        ),
        name="head_first" if first else "head_next",
    )(lengths, w, prev, *pieces)


def loss_kernel(slabs_ref, lens_ref, pairs_ref, margin_ref, logp_ref, loss_ref, z_ref):
    responses = lens_ref.shape[0]
    devices = slabs_ref.shape[0]
    top = slabs_ref[0, 0:responses, :]
    for d in range(1, devices):
        top = jnp.maximum(top, slabs_ref[d, 0:responses, :])
    total = jnp.zeros_like(top)
    picked = jnp.zeros_like(top)
    for d in range(devices):
        total = total + jnp.exp(slabs_ref[d, 0:responses, :] - top)
        picked = picked + slabs_ref[d, responses : 2 * responses, :]
    log_norm = top + jnp.log(total)
    row = lax.broadcasted_iota(jnp.int32, (responses, LANES), 0)
    lane = lax.broadcasted_iota(jnp.int32, (responses, LANES), 1)
    lens = jnp.zeros((responses, LANES), jnp.int32)
    count = jnp.int32(0)
    for s in range(responses):
        lens = jnp.where(row == s, lens_ref[s], lens)
        count = count + lens_ref[s]
    live = lane < lens
    logp = jnp.sum(jnp.where(live, picked - log_norm, 0.0), axis=1, keepdims=True)
    logp = jnp.broadcast_to(logp, (responses, LANES))
    square = jnp.where(live, log_norm * log_norm, 0.0)
    square = jnp.sum(jnp.sum(square, axis=1, keepdims=True), axis=0, keepdims=True)
    one = lax.broadcasted_iota(jnp.int32, (1, LANES), 1)
    margin = jnp.zeros((1, LANES), jnp.float32)
    for p in range(responses // 2):
        sign = jnp.where(row == pairs_ref[2 * p], 1.0, 0.0) - jnp.where(row == pairs_ref[2 * p + 1], 1.0, 0.0)
        diff = jnp.sum(sign * logp, axis=0, keepdims=True) - margin_ref[p]
        margin = jnp.where(one == p, diff, margin)
    line = jnp.sum(jnp.where(row == lane, logp, 0.0), axis=0, keepdims=True)
    logp_ref[...] = line
    loss_ref[...] = softplus(-pref_beta * margin)
    z_ref[...] = jnp.broadcast_to(zloss_weight * square / count.astype(jnp.float32), (1, LANES))


def loss_call(slabs, lengths, pair_map, ref_margin):
    vmem, smem = pl.BlockSpec(memory_space=pltpu.VMEM), pl.BlockSpec(memory_space=pltpu.SMEM)
    line = jax.ShapeDtypeStruct((1, LANES), jnp.float32)
    logp, loss, z = pl.pallas_call(
        loss_kernel,
        out_shape=(line, line, line),
        in_specs=[vmem, smem, smem, smem],
        out_specs=(vmem, vmem, vmem),
        name="losses",
    )(slabs, lengths, pair_map, ref_margin)
    return logp[0, : lengths.shape[0]], loss[0, : ref_margin.shape[0]], z[0, 0]


def square_device(hidden, head_weight, labels, lengths, pair_map, ref_margin):
    seq = lax.axis_size("seq")
    rows, depth = hidden.shape
    half = -(-rows // 32) * 16

    def swap(v, bit):
        return lax.ppermute(v, "seq", [(i, i ^ bit) for i in range(seq)])

    digits = jnp.stack([labels & 255, (labels >> 8) & 255, labels >> 16], axis=1)
    digits = jnp.pad(digits.astype(jnp.bfloat16), ((0, 0), (0, LANES - 3)))
    top = jnp.concatenate([hidden[:half], digits[:half]], axis=1)
    low = jnp.concatenate([hidden[half:], digits[half:]], axis=1)
    x_top, y_top = swap(top, 2), swap(top, 4)
    c_top, c_low = swap(top, 1), swap(low, 1)
    x_low, y_low = swap(low, 2), swap(low, 4)
    d_top, d_low = swap(x_top, 4), swap(y_low, 2)
    h = rows - half
    T, L = (0, half), (half, h)
    block = 512 if head_weight.shape[1] % 512 == 0 else LANES
    call = functools.partial(head_call, depth=depth, block=block, lengths=lengths)
    zero = jnp.zeros((2 * lengths.shape[0], LANES), jnp.float32)
    slab, w = call(
        metas=((0, *T), (0, *L), (1, *T), (1, *L)), w=head_weight, prev=zero,
        pieces=[top, low, c_top, c_low], first=True,
    )
    for a, b, at, bits in ((x_top, y_top, T, (2, 4)), (x_low, y_low, L, (2, 4)), (d_top, d_low, None, (6, 6))):
        ats = (T, L) if at is None else (at, at)
        metas = tuple((bit ^ c, *t) for c in (0, 1) for bit, t in zip(bits, ats))
        slab = call(metas=metas, w=w, prev=slab, pieces=[a, b, swap(a, 1), swap(b, 1)], first=False)
    both = ("seq", "vocab")
    n = lax.axis_size(both)
    slabs = lax.all_to_all(jnp.broadcast_to(slab[None], (n, *slab.shape)), both, 0, 0)
    return loss_call(slabs, lengths, pair_map, ref_margin)


def general_device(hidden, head_weight, labels, lengths, pair_map, ref_margin):
    vocab_devices = lax.axis_size("vocab")
    shard_rows = hidden.shape[0]
    columns = head_weight.shape[1]
    seq_total = lengths.shape[0]
    col_first = (lax.axis_index("seq") * vocab_devices + lax.axis_index("vocab")) * columns
    col_ids = col_first + jnp.arange(columns, dtype=jnp.int32)
    seq_ids = jnp.arange(seq_total, dtype=jnp.int32)
    logits = jnp.dot(
        lax.all_gather(hidden, "seq", axis=0, tiled=True),
        head_weight,
        preferred_element_type=jnp.float32,
    )
    local_max = jnp.max(logits, axis=1)
    local_sum = jnp.sum(jnp.exp(logits - local_max[:, None]), axis=1)
    all_labels = lax.all_gather(labels, "seq", axis=0, tiled=True)
    picked = jnp.sum(jnp.where(all_labels[:, None] == col_ids[None, :], logits, 0.0), axis=1)
    top_score = lax.pmax(local_max, ("seq", "vocab"))
    exp_total, label_logit = lax.psum(
        (local_sum * jnp.exp(local_max - top_score), picked), ("seq", "vocab")
    )
    log_norm = (top_score + jnp.log(exp_total)).reshape(seq_total, shard_rows)
    label_logit = label_logit.reshape(seq_total, shard_rows)
    live_mask = jnp.arange(shard_rows, dtype=jnp.int32)[None, :] < lengths[:, None]
    seq_logps = jnp.sum(jnp.where(live_mask, label_logit - log_norm, 0.0), axis=1)
    select = (pair_map[:, None] == seq_ids[None, :]).astype(jnp.float32)
    ordered = jnp.dot(select, seq_logps, precision=lax.Precision.HIGHEST).reshape(seq_total // 2, 2)
    pair_loss = jax.nn.softplus(-pref_beta * (ordered[:, 0] - ordered[:, 1] - ref_margin))
    live_count = jnp.sum(live_mask.astype(jnp.float32))
    z_loss = zloss_weight * jnp.sum(jnp.where(live_mask, log_norm * log_norm, 0.0)) / live_count
    return (seq_logps, pair_loss, z_loss)


def solution(mesh):
    placed = (P("seq", None), P(None, ("seq", "vocab")), P("seq"), P(), P(), P())
    square = mesh.shape["seq"] == 8
    return jax.shard_map(
        square_device if square else general_device,
        mesh=mesh, in_specs=placed, out_specs=(P(), P(), P()), check_vma=False,
    )
```
